256 devices in a mesh: cls: 8 (over x, y_hi), str: 32 (over z, y_lo, core).
Axes of the slice: x: 4, y: 4 (y_hi: 2, y_lo: 2; y = y_hi * 2 + y_lo), z: 8, core: 2. Of those that a mesh axis runs over, the one named last changes fastest.
Arguments:
- first_factor_tiles: float32 [8, 1024, 2, 4, 1024], P(None, ('cls', 'str')), may hold values from -6 to 6
- b_blocks: float32 [8, 1024, 2, 4, 512], P(None, ('cls', 'str')), may hold values from -0.0625 to 0.0625
Outputs:
- c_blocks: float32 [8, 1024, 2, 4, 512], P(None, ('cls', 'str'))
The draws below stay inside these ranges and needn't reach their ends.
All inputs are finite; a program needn't handle non-finite values.
Results may differ from the reference program's by a relative error of at most 0.0003.
Values sent between devices are 32-bit elements; how exact they have to be, the bound alone decides.
A program may use at most 64 MiB of HBM per device.

```python
import jax
import jax.numpy as jnp
import numpy as np
from jax import lax

N = 8192
Q = 1024
QC = 512


def block_levels(key, extent, split, low, largest):
    level = 1.0
    for position, parts in split:
        draws = jax.random.uniform(jax.random.fold_in(jax.random.fold_in(key, 6), position), (parts,), jnp.float32, low / len(split), largest / len(split))
        level = level * jnp.repeat(jnp.exp(draws), extent[position] // parts).reshape((-1,) + (1,) * (len(extent) - 1 - position))
    return level


def scatter_about(key, dims, width, bound, shards=(), kind=jnp.bfloat16):
    drawn = width * jax.random.normal(key, dims, jnp.float32)
    if shards:
        drawn = drawn * block_levels(key, dims, shards, -0.22, 0.18)
    return jnp.clip(drawn, -bound, bound).astype(kind)


def setup_inputs(seed: int = 0) -> dict:
    key_of = jax.random.split(jax.random.key(seed), 3)
    return {
        "first_factor_tiles": scatter_about(key_of[0], (8, Q, 2, 4, Q), 1.0, 6.0, ((1, 256),), jnp.float32),
        "b_blocks": scatter_about(key_of[1], (8, Q, 2, 4, QC), N ** -0.5, 0.0625, ((1, 256),), jnp.float32),
    }


def strassen_weight_lists():
    left_base = np.array([[1, 0, 0, 0], [0, 1, 0, 0], [1, 1, -1, -1], [0, 0, 0, 1], [0, 0, 1, 1], [-1, 0, 1, 1], [1, 0, -1, 0]], np.float32)
    right_base_matrix = np.array([[1, 0, 0, 0], [0, 0, 1, 0], [0, 0, 0, 1], [1, -1, -1, 1], [-1, 1, 0, 0], [1, -1, 0, 1], [0, -1, 0, 1]], np.float32)
    product_grid_start = np.array([[1, 1, 0, 0, 0, 0, 0], [1, 0, 1, 0, 1, 1, 0], [1, 0, 0, -1, 0, 1, 1], [1, 0, 0, 0, 1, 1, 1]], np.float32)
    left_split = left_base.reshape(7, 2, 2)
    right_split = right_base_matrix.reshape(7, 2, 2)
    outer_split = product_grid_start.reshape(2, 2, 7)
    left_table = (left_split[:, None, :, None, :, None] * left_split[None, :, None, :, None, :]).reshape(49, 4, 4)
    right_table = (right_split[:, None, :, None, :, None] * right_split[None, :, None, :, None, :]).reshape(49, 4, 4)
    outer_table = (outer_split[:, None, :, None, :, None] * outer_split[None, :, None, :, None, :]).reshape(4, 4, 49)
    return left_table, right_table, outer_table


def reference(first_factor_tiles, b_blocks):
    first_factor_host_grid, second_factor_host_grid, product_host_grid = strassen_weight_lists()
    left_table = jnp.asarray(first_factor_host_grid).astype(first_factor_tiles.dtype)
    right_table = jnp.asarray(second_factor_host_grid).astype(first_factor_tiles.dtype)
    outer_table = jnp.asarray(product_host_grid).astype(first_factor_tiles.dtype)
    product_ids = np.arange(8)
    inner_halves = product_ids // 4
    row_half_split = (product_ids // 2) % 2
    col_halves = product_ids % 2
    a_six = first_factor_tiles.reshape(2, 4, Q, 2, 4, Q)
    b_six = b_blocks.reshape(2, 4, Q, 2, 4, QC)
    left_stack = a_six[row_half_split, :, :, inner_halves]
    right_stack = b_six[inner_halves, :, :, col_halves]
    highest = lax.Precision.HIGHEST

    def leaf_product(pair):
        x_quad, y_quad = pair
        left_leaves = jnp.einsum('mac,aqcr->mqr', left_table, x_quad, precision=highest)
        right_leaves = jnp.einsum('mac,aqcr->mqr', right_table, y_quad, precision=highest)
        leaf_out = jnp.einsum('mqk,mkr->mqr', left_leaves, right_leaves, precision=highest)
        return jnp.einsum('acm,mqr->aqcr', outer_table, leaf_out, precision=highest)

    partials = lax.map(leaf_product, (left_stack, right_stack))
    partials = partials.reshape(2, 2, 2, 4, Q, 4, QC)
    summed = partials[0] + partials[1]
    summed = jnp.transpose(summed, (0, 2, 3, 1, 4, 5))
    return summed.reshape(8, Q, 2, 4, QC)
```

```python
import functools

import jax
import jax.numpy as jnp
from jax import lax
from jax.experimental import pallas as pl
from jax.experimental.pallas import tpu as pltpu
from jax.sharding import PartitionSpec as P

MESH = pl.DeviceIdType.MESH
COLUMN_PARTS = 2


class Plan:
    def __init__(self, nx, ny, nz, nc):
        self.nx, self.ny, self.nz, self.nc = nx, ny, nz, nc
        self.yl = min(2, ny)
        self.yh = ny // self.yl
        self.nyc = ny * nc

    def here(self):
        cls, sub = lax.axis_index("cls"), lax.axis_index("str")
        core = lax.rem(sub, self.nc)
        low = lax.rem(sub // self.nc, self.yl)
        z = sub // (self.nc * self.yl)
        x, high = cls // self.yh, lax.rem(cls, self.yh)
        return x, high * self.yl + low, z, core

    def device(self, x, y, z, core):
        return (
            x * self.yh + y // self.yl,
            (z * self.yl + lax.rem(y, self.yl)) * self.nc + core,
        )


def split_bf16(value):
    high = value.astype(jnp.bfloat16)
    low = (value - high.astype(jnp.float32)).astype(jnp.bfloat16)
    return high, low


def kernel(plan, a_ref, b_ref, c_ref, at, bt, ah, al, bh, bl, part, turn, got, total, back, send, recv):
    nx, ny, nz, nc, nyc = plan.nx, plan.ny, plan.nz, plan.nc, plan.nyc
    x, y, z, core = plan.here()
    yc = y * nc + core
    count = [0]

    def xmod(k):
        return lax.rem(x + (k + 4 * nx), nx)

    def ymod(k):
        return lax.rem(y + (k + 4 * ny), ny)

    def zmod(k):
        return lax.rem(z + (k + 4 * nz), nz)

    def ycmod(k):
        return lax.rem(yc + (k + 4 * nyc), nyc)

    def yc_device(k):
        other = ycmod(k)
        return plan.device(x, other // nc, z, lax.rem(other, nc))

    started = []

    def push(src, dst, device):
        k = count[0]
        count[0] += 1
        copy = pltpu.make_async_remote_copy(
            src_ref=src,
            dst_ref=dst,
            send_sem=send.at[k],
            recv_sem=recv.at[k],
            device_id=device,
            device_id_type=MESH,
        )
        copy.start()
        started.append(copy)
        return copy

    barrier = pltpu.get_barrier_semaphore()
    friends = [plan.device(xmod(k), y, z, core) for k in range(1, nx)]
    friends += [yc_device(k) for k in range(1, nyc)]
    if nz > 1:
        friends += [plan.device(x, y, zmod(1), core), plan.device(x, y, zmod(-1), core)]
    for friend in friends:
        pl.semaphore_signal(barrier, inc=1, device_id=friend, device_id_type=MESH)
    pl.semaphore_wait(barrier, len(friends))

    x_next, x_prev = plan.device(xmod(1), y, z, core), plan.device(xmod(-1), y, z, core)
    y_next, y_prev = plan.device(x, ymod(1), z, core), plan.device(x, ymod(-1), z, core)
    z_next, z_prev = plan.device(x, y, zmod(1), core), plan.device(x, y, zmod(-1), core)

    b_in = [push(b_ref.at[ycmod(k)], bt.at[z, yc], yc_device(k)) for k in range(1, nyc)]
    order = [k for k in (1, 3, 2) if k < nx]
    a_in = {k: push(a_ref.at[xmod(k)], at.at[x, yc], plan.device(xmod(k), y, z, core)) for k in order}
    bt[z, yc] = b_ref[yc]

    def a_source(k, ys):
        if k == 0 and ys == 0:
            return a_ref.at[x]
        return at.at[xmod(-k), ymod(ys) * nc + core]

    near, far, pair = {}, {}, {}

    def spread(k):
        src = a_source(k, 0)
        dst = at.at[xmod(-k), yc]
        if ny > 1:
            near[k, -1] = push(src, dst, y_next)
            near[k, 1] = push(src, dst, y_prev)
        give_partner(k, 0)

    def give_partner(k, ys):
        if nc > 1:
            there = plan.device(x, y, z, 1 - core)
            pair[k, ys] = push(a_source(k, ys), at.at[xmod(-k), ymod(ys) * nc + core], there)

    def cut_a(k, ys, own):
        other = core if own else 1 - core
        slot = ymod(ys) * nc + other
        xs = xmod(-k)
        rows = pl.ds(pl.multiple_of(slot * 32, 32), 32)
        value = a_ref[x] if own and k == 0 and ys == 0 else at[xs, slot]
        high, low = split_bf16(value)
        ah[xs, rows, :] = high
        al[xs, rows, :] = low

    depth = a_ref.shape[2] // 8
    group = plan.yl * nc

    def cut_b(zs, half):
        def one(b, _):
            rows = bt[zs, pl.ds(half * group, group), b].reshape(group * 4, bt.shape[4])
            high, low = split_bf16(rows)
            first = b * depth + half * (depth // plan.yh) + zs * (group * 4)
            where = pl.ds(pl.multiple_of(first, group * 4), group * 4)
            bh[where, :] = high
            bl[where, :] = low
            return 0

        lax.fori_loop(0, 8, one, 0)

    rings = {}

    def ring(direction, half, hop):
        held = zmod(-direction * (hop - 1))
        there = bt.at[held, pl.ds(half * group, group)]
        rings[direction, half, hop] = push(there, there, z_next if direction == 1 else z_prev)

    def last_hop(direction, half):
        long = (half == 0) == (direction == 1)
        return nz // 2 if long else (nz - 1) // 2

    halves = range(plan.yh)
    if plan.yh == 1:
        def last_hop(direction, half):
            return nz // 2 if direction == 1 else (nz - 1) // 2

    events = []

    def at_time(when, act):
        events.append((when, len(events), act))

    def b_arrived():
        for copy in b_in:
            copy.wait_recv()
        if nz > 1:
            for half in halves:
                for direction in (1, -1):
                    ring(direction, half, 1)
        for half in halves:
            cut_b(z, half)

    def ring_arrived(direction, half, hop):
        rings[direction, half, hop].wait_recv()
        if hop < last_hop(direction, half):
            ring(direction, half, hop + 1)
        cut_b(zmod(-direction * hop), half)

    def x_arrived(k):
        a_in[k].wait_recv()
        spread(k)
        cut_a(k, 0, True)

    def near_arrived(k, ys):
        near[k, ys].wait_recv()
        if ny == 4 and (ys == -1) == (k in (0, 3)):
            src = a_source(k, ys)
            far[k] = push(src, src, y_next if ys == -1 else y_prev)
        give_partner(k, ys)
        cut_a(k, ys, True)

    def far_arrived(k):
        far[k].wait_recv()
        give_partner(k, 2)
        cut_a(k, 2, True)

    def pair_arrived(k, ys):
        pair[k, ys].wait_recv()
        cut_a(k, ys, False)

    spread(0)
    cut_a(0, 0, True)
    at_time(5.0, b_arrived)
    ready = {0: 3.0, 1: 9.0, 3: 9.2, 2: 15.0}
    sent_at = {0: 10.0, 1: 17.0, 3: 23.0, 2: 34.0}
    far_at = {0: 29.0, 1: 29.2, 3: 40.0, 2: 41.0}
    for k in [0, *order]:
        if k:
            at_time(ready[k], functools.partial(x_arrived, k))
        if nc > 1:
            at_time(ready[k] + 3.0, functools.partial(pair_arrived, k, 0))
        if ny > 1:
            for ys in (-1, 1):
                at_time(sent_at[k], functools.partial(near_arrived, k, ys))
                if nc > 1:
                    at_time(sent_at[k] + 3.0, functools.partial(pair_arrived, k, ys))
        if ny == 4:
            at_time(far_at[k], functools.partial(far_arrived, k))
            if nc > 1:
                at_time(far_at[k] + 3.0, functools.partial(pair_arrived, k, 2))
    if nz > 1:
        for half in halves:
            for direction in (1, -1):
                for hop in range(1, last_hop(direction, half) + 1):
                    first = half if direction == 1 else 1 - half
                    at_time(7.0 + 5.5 * first + 11.0 * hop - 5.0, functools.partial(ring_arrived, direction, half, hop))
    for _, _, act in sorted(events, key=lambda e: e[:2]):
        act()

    width = bh.shape[1] // COLUMN_PARTS
    mid = nyc // 2
    lower, upper = pl.ds(0, mid), pl.ds(mid, nyc - mid)

    def product(n, k):
        xs = xmod(k)
        cols = pl.ds(n * width, width)
        right_high, right_low = bh[:, cols], bl[:, cols]
        left_high = ah[xs]
        value = jnp.dot(left_high, right_high, preferred_element_type=jnp.float32)
        value += jnp.dot(left_high, right_low, preferred_element_type=jnp.float32)
        value += jnp.dot(al[xs], right_high, preferred_element_type=jnp.float32)
        part[n, k] = value.reshape(nyc, 32, width)

    steps = {}
    for n in range(COLUMN_PARTS):
        if nx == 4:
            product(n, 2)
            steps[n, "turn", 0] = push(part.at[n, 2, lower], turn.at[n, 0], x_next)
            steps[n, "turn", 1] = push(part.at[n, 2, upper], turn.at[n, 1], x_prev)
            product(n, 1)
            steps[n, "got", 0, 1] = push(part.at[n, 1, upper], got.at[n, 0, upper], x_next)
            product(n, 3)
            steps[n, "got", 1, 0] = push(part.at[n, 3, lower], got.at[n, 1, lower], x_prev)
        product(n, 0)

    def pass_on(n):
        if nx == 4:
            steps[n, "turn", 0].wait_recv()
            part[n, 1, lower] += turn[n, 0]
            steps[n, "turn", 1].wait_recv()
            part[n, 3, upper] += turn[n, 1]
            steps[n, "got", 0, 0] = push(part.at[n, 1, lower], got.at[n, 0, lower], x_next)
            steps[n, "got", 1, 1] = push(part.at[n, 3, upper], got.at[n, 1, upper], x_prev)

    def finish(n):
        value = part[n, 0]
        if nx == 4:
            for side in (0, 1):
                for half in (0, 1):
                    steps[n, "got", side, half].wait_recv()
            value = value + got[n, 0] + got[n, 1]
        total[n] = value
        back[yc, n] = total[n, yc]
        steps[n, "back"] = [push(total.at[n, ycmod(k)], back.at[yc, n], yc_device(k)) for k in range(1, nyc)]

    for n in range(COLUMN_PARTS):
        pass_on(n)
    for n in range(COLUMN_PARTS):
        finish(n)
    for n in range(COLUMN_PARTS):
        for copy in steps[n, "back"]:
            copy.wait_recv()
    c_ref[...] = back[...]
    for copy in started:
        copy.wait_send()


def exchange_product(plan, a_parts, b_parts):
    nx, nz, nyc = plan.nx, plan.nz, plan.nyc
    inner, wide = a_parts.shape[2], b_parts.shape[3]
    width = wide // COLUMN_PARTS
    f32, bf16 = jnp.float32, jnp.bfloat16
    return pl.pallas_call(
        functools.partial(kernel, plan),
        out_shape=jax.ShapeDtypeStruct((nyc, COLUMN_PARTS, 32, width), f32),
        in_specs=[pl.BlockSpec(memory_space=pltpu.VMEM)] * 2,
        out_specs=pl.BlockSpec(memory_space=pltpu.VMEM),
        scratch_shapes=[
            pltpu.VMEM((nx, nyc, 32, inner), f32),
            pltpu.VMEM((nz, nyc, 8, 4, wide), f32),
            pltpu.VMEM((nx, nyc * 32, inner), bf16),
            pltpu.VMEM((nx, nyc * 32, inner), bf16),
            pltpu.VMEM((inner, wide), bf16),
            pltpu.VMEM((inner, wide), bf16),
            pltpu.VMEM((COLUMN_PARTS, nx, nyc, 32, width), f32),
            pltpu.VMEM((COLUMN_PARTS, 2, nyc // 2, 32, width), f32),
            pltpu.VMEM((COLUMN_PARTS, 2, nyc, 32, width), f32),
            pltpu.VMEM((COLUMN_PARTS, nyc, 32, width), f32),
            pltpu.VMEM((nyc, COLUMN_PARTS, 32, width), f32),
            pltpu.SemaphoreType.DMA((128,)),
            pltpu.SemaphoreType.DMA((128,)),
        ],
        compiler_params=pltpu.CompilerParams(
            collective_id=0, has_side_effects=True, vmem_limit_bytes=60 * 1024 * 1024
        ),
    )(a_parts, b_parts)


def local(plan, first_factor_tiles, b_blocks):
    b, i, h, c, r = first_factor_tiles.shape
    a_parts = first_factor_tiles.reshape(b * i, h * c, plan.nx, r // plan.nx)
    a_parts = jnp.transpose(a_parts, (2, 0, 1, 3)).reshape(plan.nx, b * i, h * c * r // plan.nx)
    wide = b_blocks.shape[4]
    b_parts = jnp.transpose(b_blocks.reshape(b, i, h * c, wide), (2, 0, 1, 3))
    out = exchange_product(plan, a_parts, b_parts)
    out = out.reshape(h, c, COLUMN_PARTS, b, i, wide // COLUMN_PARTS)
    return jnp.transpose(out, (3, 4, 0, 1, 2, 5)).reshape(b, i, h, c, wide)


def solution(mesh):
    plan = Plan(4, 4, mesh.shape["str"] // 4, 2)
    spec = P(None, ("cls", "str"), None, None, None)
    return jax.shard_map(
        functools.partial(local, plan), mesh=mesh, in_specs=(spec, spec), out_specs=spec, check_vma=False
    )
```

```python
import functools

import jax
import jax.numpy as jnp
from jax import lax
from jax.experimental import pallas as pl
from jax.experimental.pallas import tpu as pltpu
from jax.sharding import PartitionSpec as P

MESH = pl.DeviceIdType.MESH
WIDTHS = (384, 128)
LAG, CUT_A, CUT_B, DOT = 2.8, 0.2, 0.25, 0.0022
GROUPS = {
    (0, 0): ((2,), (1,), (3,), (0,)),
    (0, 1): ((2, 1), (3, 0)),
    (1, 0): ((2, 1, 3, 0),),
    (1, 1): ((2, 1, 3, 0),),
}
HOLD = (3, 2)


class Plan:
    def __init__(self, nx, ny, nz, nc):
        self.nx, self.ny, self.nz, self.nc = nx, ny, nz, nc
        self.yl = min(2, ny)
        self.yh = ny // self.yl
        self.nyc = ny * nc

    def here(self):
        cls, sub = lax.axis_index("cls"), lax.axis_index("str")
        core = lax.rem(sub, self.nc)
        low = lax.rem(sub // self.nc, self.yl)
        z = sub // (self.nc * self.yl)
        x, high = cls // self.yh, lax.rem(cls, self.yh)
        return x, high * self.yl + low, z, core

    def device(self, x, y, z, core):
        return (
            x * self.yh + y // self.yl,
            (z * self.yl + lax.rem(y, self.yl)) * self.nc + core,
        )


def split_bf16(value):
    high = value.astype(jnp.bfloat16)
    low = (value - high.astype(jnp.float32)).astype(jnp.bfloat16)
    return high, low


def kernel(plan, a_hbm, b_hbm, c_ref, asrc, at, ah, al, bsrc, bt, bhl, part, turn, got, total, back, a_in_ref, b_in_ref, load, send, recv):
    nx, ny, nz, nc, nyc = plan.nx, plan.ny, plan.nz, plan.nc, plan.nyc
    x, y, z, core = plan.here()
    yc = y * nc + core
    chunks = range(len(bt))
    widths = [ref.shape[4] for ref in bt]
    count = [0]
    started = []

    def xmod(k):
        return lax.rem(x + (k + 4 * nx), nx)

    def ymod(k):
        return lax.rem(y + (k + 4 * ny), ny)

    def zmod(k):
        return lax.rem(z + (k + 4 * nz), nz)

    def cmod(k):
        return lax.rem(core + k, nc)

    def push(src, dst, device):
        k = count[0]
        count[0] += 1
        copy = pltpu.make_async_remote_copy(
            src_ref=src,
            dst_ref=dst,
            send_sem=send.at[k],
            recv_sem=recv.at[k],
            device_id=device,
            device_id_type=MESH,
        )
        copy.start()
        started.append(copy)
        return copy

    b_load = pltpu.make_async_copy(b_hbm, b_in_ref, load.at[0])
    a_load = pltpu.make_async_copy(a_hbm, a_in_ref, load.at[1])
    b_load.start()
    a_load.start()
    barrier = pltpu.get_barrier_semaphore()
    near_first = [k for k in (1, 3, 2) if k < ny]
    others = [(k, q) for k in [0, *near_first] for q in range(nc) if k or q]
    friends = [plan.device(xmod(k), y, z, core) for k in range(1, nx)]
    friends += [plan.device(x, ymod(k), z, cmod(q)) for k, q in others]
    if nz > 1:
        friends += [plan.device(x, y, zmod(1), core), plan.device(x, y, zmod(-1), core)]
    for friend in friends:
        pl.semaphore_signal(barrier, inc=1, device_id=friend, device_id_type=MESH)

    a_ref, b_ref = a_in_ref, b_in_ref
    b_load.wait()

    nb, ni, nh, _, deep = a_ref.shape
    per_x = deep // nx
    for slot in range(nyc):
        h, c = divmod(slot, b_ref.shape[3])
        first = 0
        for n in chunks:
            bsrc[n][slot] = b_ref[:, :, h, c, first : first + widths[n]]
            first += widths[n]
    for n in chunks:
        bt[n][z, yc] = bsrc[n][yc]
    a_load.wait()
    for k in range(nx):
        for hc in range(nb):
            h, c = divmod(hc, nb // nh)
            rows = a_ref[:, :, h, c, k * per_x : (k + 1) * per_x].reshape(nb * ni, per_x)
            asrc[k, :, hc * per_x : (hc + 1) * per_x] = rows

    pl.semaphore_wait(barrier, len(friends))

    x_next, x_prev = plan.device(xmod(1), y, z, core), plan.device(xmod(-1), y, z, core)
    y_next, y_prev = plan.device(x, ymod(1), z, core), plan.device(x, ymod(-1), z, core)
    z_next, z_prev = plan.device(x, y, zmod(1), core), plan.device(x, y, zmod(-1), core)

    b_in = {}

    def send_b(n):
        for k, q in others:
            there = ymod(k) * nc + cmod(q)
            b_in[n, k, q] = push(bsrc[n].at[there], bt[n].at[z, yc], plan.device(x, ymod(k), z, cmod(q)))

    send_b(0)
    order = [k for k in (1, 3, 2) if k < nx]
    a_in = {k: push(asrc.at[xmod(k)], at.at[x, yc], plan.device(xmod(k), y, z, core)) for k in order}

    def a_source(k, ys):
        if k == 0 and ys == 0:
            return asrc.at[x]
        return at.at[xmod(-k), ymod(ys) * nc + core]

    near, far, pair = {}, {}, {}

    def spread(k):
        src = a_source(k, 0)
        dst = at.at[xmod(-k), yc]
        if ny > 1:
            near[k, 3] = push(src, dst, y_next)
            near[k, 1] = push(src, dst, y_prev)
        give_partner(k, 0)

    def give_partner(k, ys):
        if nc > 1:
            there = plan.device(x, y, z, cmod(1))
            pair[k, ys] = push(a_source(k, ys), at.at[xmod(-k), ymod(ys) * nc + core], there)

    row_parts = [[k for k in (0, 1, 3) if k < ny], [k for k in (2,) if k < ny]]
    place = {k: (j, p) for j, ks in enumerate(row_parts) for p, k in enumerate(ks)}

    def cut_a(k, ys, own):
        other = core if own else cmod(1)
        j, p = place[ys]
        where = pl.ds(pl.multiple_of((p * nc + other) * 32, 32), 32)
        value = asrc[x] if own and k == 0 and ys == 0 else at[xmod(-k), ymod(ys) * nc + other]
        high, low = split_bf16(value)
        ah[j][k, where, :] = high
        al[j][k, where, :] = low

    depth = asrc.shape[2] // nb
    group = plan.yl * nc

    def cut_b(n, zs):
        def one(b, _):
            for half in range(plan.yh):
                rows = bt[n][zs, pl.ds(half * group, group), b].reshape(group * 4, widths[n])
                high, low = split_bf16(rows)
                first = b * depth + half * (depth // plan.yh) + zs * (group * 4)
                where = pl.ds(pl.multiple_of(first, group * 4), group * 4)
                bhl[n][where, : widths[n]] = high
                bhl[n][where, widths[n] :] = low
            return 0

        lax.fori_loop(0, nb, one, 0)

    groups = {0: [(ymod(k) * nc, nc, k in (0, 1)) for k in [0, *near_first]]}
    wide = max(1, nyc // 2) if ny > 1 else nyc
    for n in chunks[1:]:
        groups[n] = [(first, wide, first == 0) for first in range(0, nyc, wide)]
    rings = {}

    def last_hop(n, g, up):
        return nz // 2 if groups[n][g][2] == up else (nz - 1) // 2

    def ring(n, g, up, hop):
        first, slots, _ = groups[n][g]
        there = bt[n].at[zmod(1 - hop if up else hop - 1), pl.ds(first, slots)]
        rings[n, g, up, hop] = push(there, there, z_next if up else z_prev)

    def b_arrived(n, g):
        keys = list(others)
        if n == 0:
            far_y = [0, *near_first][g]
            keys = [(k, q) for k, q in others if (k + far_y) % ny == 0]
        elif g:
            keys = []
        for k, q in keys:
            b_in[n, k, q].wait_recv()
        for up in (True, False):
            if last_hop(n, g, up):
                ring(n, g, up, 1)
        if g == len(groups[n]) - 1:
            cut_b(n, z)

    def ring_arrived(n, g, hop):
        for up in (True, False):
            if hop <= last_hop(n, g, up):
                rings[n, g, up, hop].wait_recv()
                if hop < last_hop(n, g, up):
                    ring(n, g, up, hop + 1)
        if g == len(groups[n]) - 1:
            cut_b(n, zmod(hop))
            if 2 * hop != nz:
                cut_b(n, zmod(-hop))

    def x_arrived(k):
        a_in[k].wait_recv()
        spread(k)
        cut_a(k, 0, True)

    def near_arrived(k, ys):
        near[k, ys].wait_recv()
        give_partner(k, ys)
        cut_a(k, ys, True)

    def pass_far(k):
        ys = 3 if k in (0, 3) else 1
        src = a_source(k, ys)
        far[k] = push(src, src, y_next if ys == 3 else y_prev)

    def far_arrived(k):
        far[k].wait_recv()
        give_partner(k, 2)
        cut_a(k, 2, True)

    def pair_arrived(k, ys):
        pair[k, ys].wait_recv()
        cut_a(k, ys, False)

    steps = {}

    def halves(j):
        slots = len(row_parts[j]) * nc
        return pl.ds(0, slots // 2), pl.ds(slots // 2, slots - slots // 2)

    def product(j, n, ds):
        width = widths[n]
        first = min((nx - d) % nx for d in ds)
        slots = len(row_parts[j]) * nc
        left_high = ah[j][first : first + len(ds)].reshape(len(ds) * slots * 32, ah[j].shape[2])
        left_low = al[j][first : first + len(ds)].reshape(len(ds) * slots * 32, ah[j].shape[2])
        both = jnp.dot(left_high, bhl[n][...], preferred_element_type=jnp.float32)
        value = jnp.dot(left_low, bhl[n][:, :width], preferred_element_type=jnp.float32)
        value = value + both[:, :width] + both[:, width:]
        value = value.reshape(len(ds), slots, 32, width)
        for d in ds:
            part[j][n][d] = value[(nx - d) % nx - first]
        for d in ds:
            send_part(j, n, d)

    def send_part(j, n, d):
        out = part[j][n]
        lower, upper = halves(j)
        if d == 2:
            steps[j, n, "turn", 0] = push(out.at[2, lower], turn[j][n].at[0, lower], x_next)
            steps[j, n, "turn", 1] = push(out.at[2, upper], turn[j][n].at[0, upper], x_prev)
        elif d == 1:
            steps[j, n, "got", 0, 1] = push(out.at[1, upper], got[j][n].at[0, upper], x_next)
        elif d == 3:
            steps[j, n, "got", 1, 0] = push(out.at[3, lower], got[j][n].at[1, lower], x_prev)

    def pass_on(j, n):
        if nx == 4:
            lower, upper = halves(j)
            out = part[j][n]
            steps[j, n, "turn", 0].wait_recv()
            out[1, lower] += turn[j][n][0, lower]
            steps[j, n, "turn", 1].wait_recv()
            out[3, upper] += turn[j][n][0, upper]
            steps[j, n, "got", 0, 0] = push(out.at[1, lower], got[j][n].at[0, lower], x_next)
            steps[j, n, "got", 1, 1] = push(out.at[3, upper], got[j][n].at[1, upper], x_prev)

    def finish(j, n):
        value = part[j][n][0]
        if nx == 4:
            for side in (0, 1):
                for half in (0, 1):
                    steps[j, n, "got", side, half].wait_recv()
            value = value + got[j][n][0] + got[j][n][1]
        total[j][n][...] = value
        for p, k in enumerate(row_parts[j]):
            for q in range(nc):
                src = total[j][n].at[p * nc + cmod(q)]
                if k or q:
                    there = plan.device(x, ymod(k), z, cmod(q))
                    steps[n, "back", k, q] = push(src, back[n].at[yc], there)
                else:
                    back[n][yc] = total[j][n][core]

    def hand_over(n):
        for k, q in others:
            steps[n, "back", k, q].wait_recv()
        first = sum(widths[:n])
        for slot in range(nyc):
            h, c = divmod(slot, c_ref.shape[3])
            c_ref[:, :, h, c, first : first + widths[n]] = back[n][slot].reshape(nb, ni, widths[n])

    acts = dict(
        send_b=send_b, b_arrived=b_arrived, ring_arrived=ring_arrived, x_arrived=x_arrived,
        near_arrived=near_arrived, pass_far=pass_far, far_arrived=far_arrived, pair_arrived=pair_arrived,
        product=product, pass_on=pass_on, finish=finish, hand_over=hand_over,
    )
    spread(0)
    cut_a(0, 0, True)
    inner = asrc.shape[2]
    plans = schedule(plan, order, near_first, groups, last_hop, row_parts, chunks, widths, inner)
    for _, act, what in plans:
        acts[act](*what)
    for copy in started:
        copy.wait_send()


def schedule(plan, order, near_first, groups, last_hop, row_parts, chunks, widths, inner):
    steps, known, free, clock = [], {"go": 0.0}, {}, [0.0]
    rate = 46.0
    piece = 32 * inner * 4 / 1024.0

    def add(act, what, deps, sends=(), cost=0.0, rank=1):
        steps.append((act, what, deps, sends, cost, rank))

    def slot(n):
        return 32 * widths[n] * 4 / 1024.0

    def b_sends(n):
        return [(("b_in", n, k, q), {0: "d", 1: "yu", 2: ("yu", "yd")[q], 3: "yd"}[k], slot(n) * (2 if k == 2 else 1)) for k in [0, *near_first] for q in range(plan.nc) if k or q]

    add("send_b", (0,), ["go"], b_sends(0), 0.0, 0)
    add("x_send", (), [("send_b", 0)], [(("x", k), {1: "xu", 2: "xu", 3: "xd"}[k], piece) for k in order], 0.0, 0)
    for n in chunks[1:]:
        add("send_b", (n,), [("x_send",), ("spread", 0)], b_sends(n), 0.0, 0)

    def spread(k):
        sends = [(("near", k, 3), "yu", piece), (("near", k, 1), "yd", piece)] if near_first else []
        return sends + ([(("pair", k, 0), "d", piece)] if plan.nc > 1 else [])

    add("spread", (0,), [("x_send",)], spread(0), CUT_A, 0)
    for k in order:
        add("x_arrived", (k,), [("x", k)], spread(k), CUT_A, 0)
    all_x = [("x_arrived", k) for k in order]
    cuts = {j: [] for j in range(2)}
    cuts[0] += [("spread", 0), *all_x]
    for k in [0, *order]:
        for ys in [0, *near_first]:
            j = 1 if ys == 2 else 0
            if ys == 2:
                near = ("near_arrived", k, 3 if k in (0, 3) else 1)
                add("pass_far", (k,), [near, *all_x], [(("far", k), "yu" if k in (0, 3) else "yd", piece)], 0.0, 0)
                add("far_arrived", (k,), [("far", k)], [(("pair", k, 2), "d", piece)] if plan.nc > 1 else [], CUT_A, 1)
                cuts[1].append(("far_arrived", k))
            elif ys:
                add("near_arrived", (k, ys), [("near", k, ys)], [(("pair", k, ys), "d", piece)] if plan.nc > 1 else [], CUT_A, 1)
                cuts[0].append(("near_arrived", k, ys))
            if plan.nc > 1:
                add("pair_arrived", (k, ys), [("pair", k, ys)], [], CUT_A, 2)
                cuts[j].append(("pair_arrived", k, ys))
    b_cuts = {n: [] for n in chunks}
    for n in chunks:
        for g, (_, slots, _) in enumerate(groups[n]):
            if n == 0:
                far_y = [0, *near_first][g]
                keys = [("b_in", n, k, q) for k in [0, *near_first] for q in range(plan.nc) if (k or q) and (k + far_y) % plan.ny == 0]
            else:
                keys = [("b_in", n, k, q) for k in [0, *near_first] for q in range(plan.nc) if k or q] + [("ring_arrived", 0, min(HOLD[0], len(groups[0]) - 1), HOLD[1])] * (plan.nz == 8)
            keys = keys or ["go"]
            if g:
                keys.append(("b_arrived", n, g - 1))
            ups = [up for up in (True, False) if last_hop(n, g, up)]
            last = g == len(groups[n]) - 1
            sends = [(("ring", n, g, up, 1), "zu" if up else "zd", slot(n) * slots) for up in ups]
            add("b_arrived", (n, g), keys, sends, CUT_B * last, 0)
            if last:
                b_cuts[n].append(("b_arrived", n, g))
            for hop in range(1, max(last_hop(n, g, True), last_hop(n, g, False)) + 1):
                keys = [("ring", n, g, up, hop) for up in ups if hop <= last_hop(n, g, up)]
                if g:
                    keys.append(("ring_arrived", n, g - 1, hop))
                sends = [(("ring", n, g, up, hop + 1), "zu" if up else "zd", slot(n) * slots) for up in ups if hop < last_hop(n, g, up)]
                add("ring_arrived", (n, g, hop), keys, sends, CUT_B * last * (1 if 2 * hop == plan.nz else 2), 0)
                if last:
                    b_cuts[n].append(("ring_arrived", n, g, hop))
    for n in chunks:
        for j in range(2):
            slots = len(row_parts[j]) * plan.nc
            if not slots:
                continue
            half = slot(n) * slots / 2
            before = cuts[j] + b_cuts[n]
            sets = [(0,)]
            if plan.nx == 4:
                sets = GROUPS[j, n]
            for ds in sets:
                columns = 256 * (-(-2 * widths[n] // 256) + -(-widths[n] // 256))
                cost = 0.25 + DOT * len(ds) * slots * 32 * columns * inner / 1e6
                sends = []
                for d in ds:
                    if d == 2:
                        sends += [(("turn", j, n, 0), "xu", half), (("turn", j, n, 1), "xd", half)]
                    elif d:
                        sends += [(("got", j, n, d, 0), "xu" if d == 1 else "xd", half)]
                add("product", (j, n, ds), before, ["late", *sends], cost, 6 + n - 0.5 * j)
                before = [*before, ("product", j, n, ds)]
            done = before[-1]
            keys = []
            if plan.nx == 4:
                add("pass_on", (j, n), [("turn", j, n, 0), ("turn", j, n, 1), ("product", j, n, next(ds for ds in sets if 3 in ds))], ["late", (("got", j, n, 1, 1), "xu", half), (("got", j, n, 3, 1), "xd", half)], 0.2, 3)
                keys = [("got", j, n, d, i) for d in (1, 3) for i in (0, 1)] + [("pass_on", j, n)]
            sends = ["late"] + [(("back", n, k, q), {0: "d", 1: "yu", 2: ("yu", "yd")[q], 3: "yd"}[k], slot(n) * (2 if k == 2 else 1)) for k in row_parts[j] for q in range(plan.nc) if k or q]
            add("finish", (j, n), [*keys, done], sends, 0.3, 3)
        ends = [("finish", j, n) for j in range(2) if row_parts[j]]
        pieces = [(k, q) for k in [0, *near_first] for q in range(plan.nc) if k or q]
        add("hand_over", (n,), [*ends, *(("back", n, *piece) for piece in pieces)], [], 0.3, 4 + n)

    out = []
    while steps:
        able = [(max(known[d] for d in s[2]), i) for i, s in enumerate(steps) if all(d in known for d in s[2])]
        now = [(steps[i][5], when, i) for when, i in able if when <= clock[0]]
        i = min(now)[2] if now else min(able)[1]
        act, what, deps, sends, cost, _ = steps.pop(i)
        clock[0] = max(clock[0], max(known[d] for d in deps)) + 0.05
        late = bool(sends) and sends[0] == "late"
        if late:
            clock[0] += cost
        for key, link, size in sends[1:] if late else sends:
            speed = 300.0 if link == "d" else rate * 1024 / 1000 * 0.98
            begun = max(clock[0], free.get(link, 0.0))
            free[link] = begun + size / speed
            known[key] = free[link] + (0.9 if link == "d" else LAG)
        if not late:
            clock[0] += cost
        known[(act, *what)] = clock[0]
        out.append((clock[0], act, what))
    first = (("send_b", (0,)), ("x_send", ()), ("spread", (0,)))
    return [(when, act, what) for when, act, what in out if (act, what) not in first]


def exchange_product(plan, widths, a_rows, b_rows):
    nx, nz, nc, nyc = plan.nx, plan.nz, plan.nc, plan.nyc
    nb, ni, nh, na, deep = a_rows.shape
    inner = nh * na * deep // nx
    f32, bf16 = jnp.float32, jnp.bfloat16
    slots = [min(3, plan.ny) * nc, nc] if plan.ny == 4 else [nyc, nc]

    def per_part(of):
        return [[pltpu.VMEM(of(s, w), f32) for w in widths] for s in slots]

    return pl.pallas_call(
        functools.partial(kernel, plan),
        out_shape=jax.ShapeDtypeStruct(b_rows.shape, f32),
        in_specs=[pl.BlockSpec(memory_space=pl.ANY)] * 2,
        out_specs=pl.BlockSpec(memory_space=pltpu.VMEM),
        scratch_shapes=[
            pltpu.VMEM((nx, 32, inner), f32),
            pltpu.VMEM((nx, nyc, 32, inner), f32),
            [pltpu.VMEM((nx, s * 32, inner), bf16) for s in slots],
            [pltpu.VMEM((nx, s * 32, inner), bf16) for s in slots],
            [pltpu.VMEM((nyc, nb, ni, w), f32) for w in widths],
            [pltpu.VMEM((nz, nyc, nb, ni, w), f32) for w in widths],
            [pltpu.VMEM((inner, 2 * w), bf16) for w in widths],
            per_part(lambda s, w: (nx, s, 32, w)),
            per_part(lambda s, w: (1, s, 32, w)),
            per_part(lambda s, w: (2, s, 32, w)),
            per_part(lambda s, w: (s, 32, w)),
            [pltpu.VMEM((nyc, 32, w), f32) for w in widths],
            pltpu.VMEM(a_rows.shape, f32),
            pltpu.VMEM(b_rows.shape, f32),
            pltpu.SemaphoreType.DMA((2,)),
            pltpu.SemaphoreType.DMA((150,)),
            pltpu.SemaphoreType.DMA((150,)),
        ],
        compiler_params=pltpu.CompilerParams(
            collective_id=0, has_side_effects=True, vmem_limit_bytes=60 * 1024 * 1024
        ),
    )(a_rows, b_rows)


def solution(mesh):
    plan = Plan(4, 4, mesh.shape["str"] // 4, 2)
    spec = P(None, ("cls", "str"), None, None, None)
    return jax.shard_map(
        functools.partial(exchange_product, plan, WIDTHS),
        mesh=mesh,
        in_specs=(spec, spec),
        out_specs=spec,
        check_vma=False,
    )
```

```python
import functools

import jax
import jax.numpy as jnp
from jax import lax
from jax.experimental import pallas as pl
from jax.experimental.pallas import tpu as pltpu
from jax.sharding import PartitionSpec as P

MESH = pl.DeviceIdType.MESH
WIDTHS = (256, 128, 128)
LAG, CUT_A, CUT_B, DOT = 2.8, 0.2, 0.25, 0.0022
GROUPS = {
    (0, 0): ((2, 1), (3, 0)),
    (0, 1): ((2, 1), (3, 0)),
    (0, 2): ((2, 1), (3, 0)),
    (1, 0): ((2, 1, 3, 0),),
    (1, 1): ((2, 1, 3, 0),),
    (1, 2): ((2, 1, 3, 0),),
}
HOLD = {1: (0, 1, 3), 2: (0, 4, 3)}


class Plan:
    def __init__(self, nx, ny, nz, nc):
        self.nx, self.ny, self.nz, self.nc = nx, ny, nz, nc
        self.yl = min(2, ny)
        self.yh = ny // self.yl
        self.nyc = ny * nc

    def here(self):
        cls, sub = lax.axis_index("cls"), lax.axis_index("str")
        core = lax.rem(sub, self.nc)
        low = lax.rem(sub // self.nc, self.yl)
        z = sub // (self.nc * self.yl)
        x, high = cls // self.yh, lax.rem(cls, self.yh)
        return x, high * self.yl + low, z, core

    def device(self, x, y, z, core):
        return (
            x * self.yh + y // self.yl,
            (z * self.yl + lax.rem(y, self.yl)) * self.nc + core,
        )


def split_bf16(value):
    high = value.astype(jnp.bfloat16)
    low = (value - high.astype(jnp.float32)).astype(jnp.bfloat16)
    return high, low


def kernel(plan, a_hbm, b_hbm, c_ref, asrc, at, ah, al, bsrc, bt, bhl, part, turn, got, total, back, a_in_ref, b_in_ref, load, send, recv):
    nx, ny, nz, nc, nyc = plan.nx, plan.ny, plan.nz, plan.nc, plan.nyc
    x, y, z, core = plan.here()
    yc = y * nc + core
    chunks = range(len(bt))
    widths = [ref.shape[4] for ref in bt]
    count = [0]
    started = []

    def xmod(k):
        return lax.rem(x + (k + 4 * nx), nx)

    def ymod(k):
        return lax.rem(y + (k + 4 * ny), ny)

    def zmod(k):
        return lax.rem(z + (k + 4 * nz), nz)

    def cmod(k):
        return lax.rem(core + k, nc)

    def push(src, dst, device):
        k = count[0]
        count[0] += 1
        copy = pltpu.make_async_remote_copy(
            src_ref=src,
            dst_ref=dst,
            send_sem=send.at[k],
            recv_sem=recv.at[k],
            device_id=device,
            device_id_type=MESH,
        )
        copy.start()
        started.append(copy)
        return copy

    b_load = pltpu.make_async_copy(b_hbm, b_in_ref, load.at[0])
    a_load = pltpu.make_async_copy(a_hbm, a_in_ref, load.at[1])
    b_load.start()
    a_load.start()
    barrier = pltpu.get_barrier_semaphore()
    near_first = [k for k in (1, 3, 2) if k < ny]
    others = [(k, q) for k in [0, *near_first] for q in range(nc) if k or q]
    friends = [plan.device(xmod(k), y, z, core) for k in range(1, nx)]
    friends += [plan.device(x, ymod(k), z, cmod(q)) for k, q in others]
    if nz > 1:
        friends += [plan.device(x, y, zmod(1), core), plan.device(x, y, zmod(-1), core)]
    for friend in friends:
        pl.semaphore_signal(barrier, inc=1, device_id=friend, device_id_type=MESH)

    a_ref, b_ref = a_in_ref, b_in_ref
    b_load.wait()

    nb, ni, nh, _, deep = a_ref.shape
    per_x = deep // nx
    for slot in range(nyc):
        h, c = divmod(slot, b_ref.shape[3])
        first = 0
        for n in chunks:
            bsrc[n][slot] = b_ref[:, :, h, c, first : first + widths[n]]
            first += widths[n]
    for n in chunks:
        bt[n][z, yc] = bsrc[n][yc]
    a_load.wait()
    for k in range(nx):
        for hc in range(nb):
            h, c = divmod(hc, nb // nh)
            rows = a_ref[:, :, h, c, k * per_x : (k + 1) * per_x].reshape(nb * ni, per_x)
            asrc[k, :, hc * per_x : (hc + 1) * per_x] = rows

    pl.semaphore_wait(barrier, len(friends))

    x_next, x_prev = plan.device(xmod(1), y, z, core), plan.device(xmod(-1), y, z, core)
    y_next, y_prev = plan.device(x, ymod(1), z, core), plan.device(x, ymod(-1), z, core)
    z_next, z_prev = plan.device(x, y, zmod(1), core), plan.device(x, y, zmod(-1), core)

    b_in = {}

    def send_b(n):
        for k, q in others:
            there = ymod(k) * nc + cmod(q)
            b_in[n, k, q] = push(bsrc[n].at[there], bt[n].at[z, yc], plan.device(x, ymod(k), z, cmod(q)))

    send_b(0)
    order = [k for k in (1, 3, 2) if k < nx]
    a_in = {k: push(asrc.at[xmod(k)], at.at[x, yc], plan.device(xmod(k), y, z, core)) for k in order}

    def a_source(k, ys):
        if k == 0 and ys == 0:
            return asrc.at[x]
        return at.at[xmod(-k), ymod(ys) * nc + core]

    near, far, pair = {}, {}, {}

    def spread(k):
        src = a_source(k, 0)
        dst = at.at[xmod(-k), yc]
        if ny > 1:
            near[k, 3] = push(src, dst, y_next)
            near[k, 1] = push(src, dst, y_prev)
        give_partner(k, 0)

    def give_partner(k, ys):
        if nc > 1:
            there = plan.device(x, y, z, cmod(1))
            pair[k, ys] = push(a_source(k, ys), at.at[xmod(-k), ymod(ys) * nc + core], there)

    row_parts = [[k for k in (0, 1, 3) if k < ny], [k for k in (2,) if k < ny]]
    place = {k: (j, p) for j, ks in enumerate(row_parts) for p, k in enumerate(ks)}

    def cut_a(k, ys, own):
        other = core if own else cmod(1)
        j, p = place[ys]
        where = pl.ds(pl.multiple_of((p * nc + other) * 32, 32), 32)
        value = asrc[x] if own and k == 0 and ys == 0 else at[xmod(-k), ymod(ys) * nc + other]
        high, low = split_bf16(value)
        ah[j][k, where, :] = high
        al[j][k, where, :] = low

    depth = asrc.shape[2] // nb
    group = plan.yl * nc

    def cut_b(n, zs):
        def one(b, _):
            for half in range(plan.yh):
                rows = bt[n][zs, pl.ds(half * group, group), b].reshape(group * 4, widths[n])
                high, low = split_bf16(rows)
                first = b * depth + half * (depth // plan.yh) + zs * (group * 4)
                where = pl.ds(pl.multiple_of(first, group * 4), group * 4)
                bhl[n][where, : widths[n]] = high
                bhl[n][where, widths[n] :] = low
            return 0

        lax.fori_loop(0, nb, one, 0)

    groups = {}
    for n in chunks:
        groups[n] = [(yc, 1, True, [])]
        if nc > 1:
            groups[n].append((y * nc + cmod(1), 1, True, [(0, 1)]))
        for k in near_first:
            keys = [((ny - k) % ny, q) for q in range(nc)]
            groups[n].append((ymod(k) * nc, nc, k == 1, keys))

    rings = {}

    def last_hop(n, g, up):
        return nz // 2 if groups[n][g][2] == up else (nz - 1) // 2

    def ring(n, g, up, hop):
        first, slots = groups[n][g][:2]
        there = bt[n].at[zmod(1 - hop if up else hop - 1), pl.ds(first, slots)]
        rings[n, g, up, hop] = push(there, there, z_next if up else z_prev)

    def b_arrived(n, g):
        for k, q in groups[n][g][3]:
            b_in[n, k, q].wait_recv()
        for up in (True, False):
            if last_hop(n, g, up):
                ring(n, g, up, 1)
        if g == len(groups[n]) - 1:
            cut_b(n, z)

    def ring_arrived(n, g, hop):
        for up in (True, False):
            if hop <= last_hop(n, g, up):
                rings[n, g, up, hop].wait_recv()
                if hop < last_hop(n, g, up):
                    ring(n, g, up, hop + 1)
        if g == len(groups[n]) - 1:
            cut_b(n, zmod(hop))
            if 2 * hop != nz:
                cut_b(n, zmod(-hop))

    def x_arrived(k):
        a_in[k].wait_recv()
        spread(k)
        cut_a(k, 0, True)

    def near_arrived(k, ys):
        near[k, ys].wait_recv()
        give_partner(k, ys)
        cut_a(k, ys, True)

    def pass_far(k):
        ys = 3 if k in (0, 3) else 1
        src = a_source(k, ys)
        far[k] = push(src, src, y_next if ys == 3 else y_prev)

    def far_arrived(k):
        far[k].wait_recv()
        give_partner(k, 2)
        cut_a(k, 2, True)

    def pair_arrived(k, ys):
        pair[k, ys].wait_recv()
        cut_a(k, ys, False)

    steps = {}

    def halves(j):
        slots = len(row_parts[j]) * nc
        return pl.ds(0, slots // 2), pl.ds(slots // 2, slots - slots // 2)

    def product(j, n, ds):
        width = widths[n]
        first = min((nx - d) % nx for d in ds)
        slots = len(row_parts[j]) * nc
        left_high = ah[j][first : first + len(ds)].reshape(len(ds) * slots * 32, ah[j].shape[2])
        left_low = al[j][first : first + len(ds)].reshape(len(ds) * slots * 32, ah[j].shape[2])
        both = jnp.dot(left_high, bhl[n][...], preferred_element_type=jnp.float32)
        value = jnp.dot(left_low, bhl[n][:, :width], preferred_element_type=jnp.float32)
        value = value + both[:, :width] + both[:, width:]
        value = value.reshape(len(ds), slots, 32, width)
        for d in ds:
            part[j][n][d] = value[(nx - d) % nx - first]
        for d in ds:
            send_part(j, n, d)

    def send_part(j, n, d):
        out = part[j][n]
        lower, upper = halves(j)
        if d == 2:
            steps[j, n, "turn", 0] = push(out.at[2, lower], turn[j][n].at[0, lower], x_next)
            steps[j, n, "turn", 1] = push(out.at[2, upper], turn[j][n].at[0, upper], x_prev)
        elif d == 1:
            steps[j, n, "got", 0, 1] = push(out.at[1, upper], got[j][n].at[0, upper], x_next)
        elif d == 3:
            steps[j, n, "got", 1, 0] = push(out.at[3, lower], got[j][n].at[1, lower], x_prev)

    def pass_on(j, n):
        if nx == 4:
            lower, upper = halves(j)
            out = part[j][n]
            steps[j, n, "turn", 0].wait_recv()
            out[1, lower] += turn[j][n][0, lower]
            steps[j, n, "turn", 1].wait_recv()
            out[3, upper] += turn[j][n][0, upper]
            steps[j, n, "got", 0, 0] = push(out.at[1, lower], got[j][n].at[0, lower], x_next)
            steps[j, n, "got", 1, 1] = push(out.at[3, upper], got[j][n].at[1, upper], x_prev)

    def finish(j, n):
        value = part[j][n][0]
        if nx == 4:
            for side in (0, 1):
                for half in (0, 1):
                    steps[j, n, "got", side, half].wait_recv()
            value = value + got[j][n][0] + got[j][n][1]
        total[j][n][...] = value
        for p, k in enumerate(row_parts[j]):
            for q in range(nc):
                src = total[j][n].at[p * nc + cmod(q)]
                if k or q:
                    there = plan.device(x, ymod(k), z, cmod(q))
                    steps[n, "back", k, q] = push(src, back[n].at[yc], there)
                else:
                    back[n][yc] = total[j][n][core]

    def hand_over(n):
        for k, q in others:
            steps[n, "back", k, q].wait_recv()
        first = sum(widths[:n])
        for slot in range(nyc):
            h, c = divmod(slot, c_ref.shape[3])
            c_ref[:, :, h, c, first : first + widths[n]] = back[n][slot].reshape(nb, ni, widths[n])

    acts = dict(
        send_b=send_b, b_arrived=b_arrived, ring_arrived=ring_arrived, x_arrived=x_arrived,
        near_arrived=near_arrived, pass_far=pass_far, far_arrived=far_arrived, pair_arrived=pair_arrived,
        product=product, pass_on=pass_on, finish=finish, hand_over=hand_over,
    )
    spread(0)
    cut_a(0, 0, True)
    inner = asrc.shape[2]
    plans = schedule(plan, order, near_first, groups, last_hop, row_parts, chunks, widths, inner)
    for _, act, what in plans:
        acts[act](*what)
    for copy in started:
        copy.wait_send()


def schedule(plan, order, near_first, groups, last_hop, row_parts, chunks, widths, inner):
    steps, known, free, clock = [], {"go": 0.0}, {}, [0.0]
    rate = 46.0
    piece = 32 * inner * 4 / 1024.0

    def add(act, what, deps, sends=(), cost=0.0, rank=1):
        steps.append((act, what, deps, sends, cost, rank))

    def slot(n):
        return 32 * widths[n] * 4 / 1024.0

    def b_sends(n):
        return [(("b_in", n, k, q), {0: "d", 1: "yu", 2: ("yu", "yd")[q], 3: "yd"}[k], slot(n) * (2 if k == 2 else 1)) for k in [0, *near_first] for q in range(plan.nc) if k or q]

    add("send_b", (0,), ["go"], b_sends(0), 0.0, 0)
    add("x_send", (), [("send_b", 0)], [(("x", k), {1: "xu", 2: "xu", 3: "xd"}[k], piece) for k in order], 0.0, 0)
    for n in chunks[1:]:
        add("send_b", (n,), [("x_send",), ("spread", 0)], b_sends(n), 0.0, 0)

    def spread(k):
        sends = [(("near", k, 3), "yu", piece), (("near", k, 1), "yd", piece)] if near_first else []
        return sends + ([(("pair", k, 0), "d", piece)] if plan.nc > 1 else [])

    add("spread", (0,), [("x_send",)], spread(0), CUT_A, 0)
    for k in order:
        add("x_arrived", (k,), [("x", k)], spread(k), CUT_A, 0)
    all_x = [("x_arrived", k) for k in order]
    cuts = {j: [] for j in range(2)}
    cuts[0] += [("spread", 0), *all_x]
    for k in [0, *order]:
        for ys in [0, *near_first]:
            j = 1 if ys == 2 else 0
            if ys == 2:
                near = ("near_arrived", k, 3 if k in (0, 3) else 1)
                add("pass_far", (k,), [near, *all_x], [(("far", k), "yu" if k in (0, 3) else "yd", piece)], 0.0, 0)
                add("far_arrived", (k,), [("far", k)], [(("pair", k, 2), "d", piece)] if plan.nc > 1 else [], CUT_A, 1)
                cuts[1].append(("far_arrived", k))
            elif ys:
                add("near_arrived", (k, ys), [("near", k, ys)], [(("pair", k, ys), "d", piece)] if plan.nc > 1 else [], CUT_A, 1)
                cuts[0].append(("near_arrived", k, ys))
            if plan.nc > 1:
                add("pair_arrived", (k, ys), [("pair", k, ys)], [], CUT_A, 2)
                cuts[j].append(("pair_arrived", k, ys))
    b_cuts = {n: [] for n in chunks}
    for n in chunks:
        for g, (_, slots, _, pieces) in enumerate(groups[n]):
            keys = [("send_b", n), *(("b_in", n, *piece) for piece in pieces)]
            if n and plan.nz == 8 and plan.ny == 4:
                keys.append(("ring_arrived", *HOLD[n]))
            if g:
                keys.append(("b_arrived", n, g - 1))
            ups = [up for up in (True, False) if last_hop(n, g, up)]
            last = g == len(groups[n]) - 1
            sends = [(("ring", n, g, up, 1), "zu" if up else "zd", slot(n) * slots) for up in ups]
            add("b_arrived", (n, g), keys, sends, CUT_B * last, 0)
            if last:
                b_cuts[n].append(("b_arrived", n, g))
            for hop in range(1, max(last_hop(n, g, True), last_hop(n, g, False)) + 1):
                keys = [("ring", n, g, up, hop) for up in ups if hop <= last_hop(n, g, up)]
                if g:
                    keys.append(("ring_arrived", n, g - 1, hop))
                sends = [(("ring", n, g, up, hop + 1), "zu" if up else "zd", slot(n) * slots) for up in ups if hop < last_hop(n, g, up)]
                add("ring_arrived", (n, g, hop), keys, sends, CUT_B * last * (1 if 2 * hop == plan.nz else 2), 0)
                if last:
                    b_cuts[n].append(("ring_arrived", n, g, hop))
    for n in chunks:
        for j in range(2):
            slots = len(row_parts[j]) * plan.nc
            if not slots:
                continue
            half = slot(n) * slots / 2
            before = cuts[j] + b_cuts[n]
            sets = [(0,)]
            if plan.nx == 4:
                sets = GROUPS[j, n]
            for ds in sets:
                columns = 256 * (-(-2 * widths[n] // 256) + -(-widths[n] // 256))
                cost = 0.25 + DOT * len(ds) * slots * 32 * columns * inner / 1e6
                sends = []
                for d in ds:
                    if d == 2:
                        sends += [(("turn", j, n, 0), "xu", half), (("turn", j, n, 1), "xd", half)]
                    elif d:
                        sends += [(("got", j, n, d, 0), "xu" if d == 1 else "xd", half)]
                add("product", (j, n, ds), before, ["late", *sends], cost, 6 + n - 0.5 * j)
                before = [*before, ("product", j, n, ds)]
            done = before[-1]
            keys = []
            if plan.nx == 4:
                add("pass_on", (j, n), [("turn", j, n, 0), ("turn", j, n, 1), ("product", j, n, next(ds for ds in sets if 3 in ds))], ["late", (("got", j, n, 1, 1), "xu", half), (("got", j, n, 3, 1), "xd", half)], 0.2, 3)
                keys = [("got", j, n, d, i) for d in (1, 3) for i in (0, 1)] + [("pass_on", j, n)]
            sends = ["late"] + [(("back", n, k, q), {0: "d", 1: "yu", 2: ("yu", "yd")[q], 3: "yd"}[k], slot(n) * (2 if k == 2 else 1)) for k in row_parts[j] for q in range(plan.nc) if k or q]
            add("finish", (j, n), [*keys, done], sends, 0.3, 3)
        ends = [("finish", j, n) for j in range(2) if row_parts[j]]
        pieces = [(k, q) for k in [0, *near_first] for q in range(plan.nc) if k or q]
        add("hand_over", (n,), [*ends, *(("back", n, *piece) for piece in pieces)], [], 0.3, 4 + n)

    out = []
    while steps:
        able = [(max(known[d] for d in s[2]), i) for i, s in enumerate(steps) if all(d in known for d in s[2])]
        now = [(steps[i][5], when, i) for when, i in able if when <= clock[0]]
        i = min(now)[2] if now else min(able)[1]
        act, what, deps, sends, cost, _ = steps.pop(i)
        clock[0] = max(clock[0], max(known[d] for d in deps)) + 0.05
        late = bool(sends) and sends[0] == "late"
        if late:
            clock[0] += cost
        for key, link, size in sends[1:] if late else sends:
            speed = 300.0 if link == "d" else rate * 1024 / 1000 * 0.98
            begun = max(clock[0], free.get(link, 0.0))
            free[link] = begun + size / speed
            known[key] = free[link] + (0.9 if link == "d" else LAG)
        if not late:
            clock[0] += cost
        known[(act, *what)] = clock[0]
        out.append((clock[0], act, what))
    first = (("send_b", (0,)), ("x_send", ()), ("spread", (0,)))
    return [(when, act, what) for when, act, what in out if (act, what) not in first]


def exchange_product(plan, widths, a_rows, b_rows):
    nx, nz, nc, nyc = plan.nx, plan.nz, plan.nc, plan.nyc
    nb, ni, nh, na, deep = a_rows.shape
    inner = nh * na * deep // nx
    f32, bf16 = jnp.float32, jnp.bfloat16
    slots = [min(3, plan.ny) * nc, nc] if plan.ny == 4 else [nyc, nc]

    def per_part(of):
        return [[pltpu.VMEM(of(s, w), f32) for w in widths] for s in slots]

    return pl.pallas_call(
        functools.partial(kernel, plan),
        out_shape=pltpu.VMEM(b_rows.shape, f32),
        in_specs=[pl.BlockSpec(memory_space=pl.ANY)] * 2,
        out_specs=pl.BlockSpec(memory_space=pltpu.VMEM),
        scratch_shapes=[
            pltpu.VMEM((nx, 32, inner), f32),
            pltpu.VMEM((nx, nyc, 32, inner), f32),
            [pltpu.VMEM((nx, s * 32, inner), bf16) for s in slots],
            [pltpu.VMEM((nx, s * 32, inner), bf16) for s in slots],
            [pltpu.VMEM((nyc, nb, ni, w), f32) for w in widths],
            [pltpu.VMEM((nz, nyc, nb, ni, w), f32) for w in widths],
            [pltpu.VMEM((inner, 2 * w), bf16) for w in widths],
            per_part(lambda s, w: (nx, s, 32, w)),
            per_part(lambda s, w: (1, s, 32, w)),
            per_part(lambda s, w: (2, s, 32, w)),
            per_part(lambda s, w: (s, 32, w)),
            [pltpu.VMEM((nyc, 32, w), f32) for w in widths],
            pltpu.VMEM(a_rows.shape, f32),
            pltpu.VMEM(b_rows.shape, f32),
            pltpu.SemaphoreType.DMA((2,)),
            pltpu.SemaphoreType.DMA((240,)),
            pltpu.SemaphoreType.DMA((240,)),
        ],
        compiler_params=pltpu.CompilerParams(
            collective_id=0, has_side_effects=True, vmem_limit_bytes=60 * 1024 * 1024
        ),
    )(a_rows, b_rows)


def solution(mesh):
    plan = Plan(4, 4, mesh.shape["str"] // 4, 2)
    spec = P(None, ("cls", "str"), None, None, None)
    return jax.shard_map(
        functools.partial(exchange_product, plan, WIDTHS),
        mesh=mesh,
        in_specs=(spec, spec),
        out_specs=spec,
        check_vma=False,
    )
```

```python
import functools

import jax
import jax.numpy as jnp
from jax import lax
from jax.experimental import pallas as pl
from jax.experimental.pallas import tpu as pltpu
from jax.sharding import PartitionSpec as P

MESH = pl.DeviceIdType.MESH
WIDTHS = (256, 128, 128)
LAG, CUT_A, CUT_B, DOT = 2.8, 0.2, 0.25, 0.0022
GROUPS = {
    (0, 0): ((2, 1), (3, 0)),
    (0, 1): ((2, 1), (3, 0)),
    (0, 2): ((2, 1), (3, 0)),
    (1, 0): ((2, 1, 3, 0),),
    (1, 1): ((2, 1, 3, 0),),
    (1, 2): ((2, 1, 3, 0),),
}
HOLD = {1: (0, 1, 3), 2: (0, 4, 3)}


class Plan:
    def __init__(self, nx, ny, nz, nc):
        self.nx, self.ny, self.nz, self.nc = nx, ny, nz, nc
        self.yl = min(2, ny)
        self.yh = ny // self.yl
        self.nyc = ny * nc

    def here(self):
        cls, sub = lax.axis_index("cls"), lax.axis_index("str")
        core = lax.rem(sub, self.nc)
        low = lax.rem(sub // self.nc, self.yl)
        z = sub // (self.nc * self.yl)
        x, high = cls // self.yh, lax.rem(cls, self.yh)
        return x, high * self.yl + low, z, core

    def device(self, x, y, z, core):
        return (
            x * self.yh + y // self.yl,
            (z * self.yl + lax.rem(y, self.yl)) * self.nc + core,
        )


def split_bf16(value):
    high = value.astype(jnp.bfloat16)
    low = (value - high.astype(jnp.float32)).astype(jnp.bfloat16)
    return high, low


def kernel(plan, a_hbm, b_hbm, c_ref, asrc, at, ah, al, bsrc, bt, bhl, part, turn, got, total, back, a_in_ref, b_in_ref, load, send, recv):
    nx, ny, nz, nc, nyc = plan.nx, plan.ny, plan.nz, plan.nc, plan.nyc
    x, y, z, core = plan.here()
    yc = y * nc + core
    chunks = range(len(bt))
    widths = [ref.shape[4] for ref in bt]
    count = [0]
    started = []

    def xmod(k):
        return lax.rem(x + (k + 4 * nx), nx)

    def ymod(k):
        return lax.rem(y + (k + 4 * ny), ny)

    def zmod(k):
        return lax.rem(z + (k + 4 * nz), nz)

    def cmod(k):
        return lax.rem(core + k, nc)

    def push(src, dst, device):
        k = count[0]
        count[0] += 1
        copy = pltpu.make_async_remote_copy(
            src_ref=src,
            dst_ref=dst,
            send_sem=send.at[k],
            recv_sem=recv.at[k],
            device_id=device,
            device_id_type=MESH,
        )
        copy.start()
        started.append(copy)
        return copy

    b_load = pltpu.make_async_copy(b_hbm, b_in_ref, load.at[0])
    a_load = pltpu.make_async_copy(a_hbm, a_in_ref, load.at[1])
    b_load.start()
    a_load.start()
    barrier = pltpu.get_barrier_semaphore()
    near_first = [k for k in (1, 3, 2) if k < ny]
    others = [(k, q) for k in [0, *near_first] for q in range(nc) if k or q]
    friends = [plan.device(xmod(k), y, z, core) for k in range(1, nx)]
    friends += [plan.device(x, ymod(k), z, cmod(q)) for k, q in others]
    if nz > 1:
        friends += [plan.device(x, y, zmod(1), core), plan.device(x, y, zmod(-1), core)]
    for friend in friends:
        pl.semaphore_signal(barrier, inc=1, device_id=friend, device_id_type=MESH)

    a_ref, b_ref = a_in_ref, b_in_ref
    b_load.wait()

    nb, ni, nh, _, deep = a_ref.shape
    per_x = deep // nx
    for slot in range(nyc):
        h, c = divmod(slot, b_ref.shape[3])
        first = 0
        for n in chunks:
            bsrc[n][slot] = b_ref[:, :, h, c, first : first + widths[n]]
            first += widths[n]
    for n in chunks:
        bt[n][z, yc] = bsrc[n][yc]
    a_load.wait()
    for k in range(nx):
        for hc in range(nb):
            h, c = divmod(hc, nb // nh)
            rows = a_ref[:, :, h, c, k * per_x : (k + 1) * per_x].reshape(nb * ni, per_x)
            asrc[k, :, hc * per_x : (hc + 1) * per_x] = rows

    pl.semaphore_wait(barrier, len(friends))

    x_next, x_prev = plan.device(xmod(1), y, z, core), plan.device(xmod(-1), y, z, core)
    y_next, y_prev = plan.device(x, ymod(1), z, core), plan.device(x, ymod(-1), z, core)
    z_next, z_prev = plan.device(x, y, zmod(1), core), plan.device(x, y, zmod(-1), core)

    b_in = {}

    def send_b(n):
        for k, q in others:
            there = ymod(k) * nc + cmod(q)
            b_in[n, k, q] = push(bsrc[n].at[there], bt[n].at[z, yc], plan.device(x, ymod(k), z, cmod(q)))

    send_b(0)
    order = [k for k in (1, 3, 2) if k < nx]
    a_in = {k: push(asrc.at[xmod(k)], at.at[x, yc], plan.device(xmod(k), y, z, core)) for k in order}

    def a_source(k, ys):
        if k == 0 and ys == 0:
            return asrc.at[x]
        return at.at[xmod(-k), ymod(ys) * nc + core]

    near, far, pair = {}, {}, {}

    def spread(k):
        src = a_source(k, 0)
        dst = at.at[xmod(-k), yc]
        if ny > 1:
            near[k, 3] = push(src, dst, y_next)
            near[k, 1] = push(src, dst, y_prev)
        give_partner(k, 0)

    def give_partner(k, ys):
        if nc > 1:
            there = plan.device(x, y, z, cmod(1))
            pair[k, ys] = push(a_source(k, ys), at.at[xmod(-k), ymod(ys) * nc + core], there)

    row_parts = [[k for k in (0, 1, 3) if k < ny], [k for k in (2,) if k < ny]]
    place = {k: (j, p) for j, ks in enumerate(row_parts) for p, k in enumerate(ks)}

    def cut_a(k, ys, own):
        other = core if own else cmod(1)
        j, p = place[ys]
        where = pl.ds(pl.multiple_of((p * nc + other) * 32, 32), 32)
        value = asrc[x] if own and k == 0 and ys == 0 else at[xmod(-k), ymod(ys) * nc + other]
        high, low = split_bf16(value)
        ah[j][k, where, :] = high
        al[j][k, where, :] = low

    depth = asrc.shape[2] // nb
    group = plan.yl * nc

    def cut_b(n, zs):
        def one(b, _):
            for half in range(plan.yh):
                rows = bt[n][zs, pl.ds(half * group, group), b].reshape(group * 4, widths[n])
                high, low = split_bf16(rows)
                first = b * depth + half * (depth // plan.yh) + zs * (group * 4)
                where = pl.ds(pl.multiple_of(first, group * 4), group * 4)
                bhl[n][where, : widths[n]] = high
                bhl[n][where, widths[n] :] = low
            return 0

        lax.fori_loop(0, nb, one, 0)

    groups = {}
    for n in chunks:
        groups[n] = [(yc, 1, True, [])]
        if nc > 1:
            groups[n].append((y * nc + cmod(1), 1, True, [(0, 1)]))
        for k in near_first:
            keys = [((ny - k) % ny, q) for q in range(nc)]
            groups[n].append((ymod(k) * nc, nc, k == 1, keys))

    rings = {}

    def last_hop(n, g, up):
        return nz // 2 if groups[n][g][2] == up else (nz - 1) // 2

    def ring(n, g, up, hop):
        first, slots = groups[n][g][:2]
        there = bt[n].at[zmod(1 - hop if up else hop - 1), pl.ds(first, slots)]
        rings[n, g, up, hop] = push(there, there, z_next if up else z_prev)

    def b_arrived(n, g):
        for k, q in groups[n][g][3]:
            b_in[n, k, q].wait_recv()
        for up in (True, False):
            if last_hop(n, g, up):
                ring(n, g, up, 1)
        if g == len(groups[n]) - 1:
            cut_b(n, z)

    def ring_arrived(n, g, hop):
        for up in (True, False):
            if hop <= last_hop(n, g, up):
                rings[n, g, up, hop].wait_recv()
                if hop < last_hop(n, g, up):
                    ring(n, g, up, hop + 1)
        if g == len(groups[n]) - 1:
            cut_b(n, zmod(hop))
            if 2 * hop != nz:
                cut_b(n, zmod(-hop))

    def x_arrived(k):
        a_in[k].wait_recv()
        spread(k)
        cut_a(k, 0, True)

    def near_arrived(k, ys):
        near[k, ys].wait_recv()
        give_partner(k, ys)
        cut_a(k, ys, True)

    def pass_far(k):
        ys = 3 if k in (0, 3) else 1
        src = a_source(k, ys)
        far[k] = push(src, src, y_next if ys == 3 else y_prev)

    def far_arrived(k):
        far[k].wait_recv()
        give_partner(k, 2)
        cut_a(k, 2, True)

    def pair_arrived(k, ys):
        pair[k, ys].wait_recv()
        cut_a(k, ys, False)

    steps = {}

    def halves(j):
        slots = len(row_parts[j]) * nc
        return pl.ds(0, slots // 2), pl.ds(slots // 2, slots - slots // 2)

    def product(j, n, ds):
        width = widths[n]
        first = min((nx - d) % nx for d in ds)
        slots = len(row_parts[j]) * nc
        left_high = ah[j][first : first + len(ds)].reshape(len(ds) * slots * 32, ah[j].shape[2])
        left_low = al[j][first : first + len(ds)].reshape(len(ds) * slots * 32, ah[j].shape[2])
        both = jnp.dot(left_high, bhl[n][...], preferred_element_type=jnp.float32)
        value = jnp.dot(left_low, bhl[n][:, :width], preferred_element_type=jnp.float32)
        value = value + both[:, :width] + both[:, width:]
        value = value.reshape(len(ds), slots, 32, width)
        for d in ds:
            part[j][n][d] = value[(nx - d) % nx - first]
        for d in ds:
            send_part(j, n, d)

    def send_part(j, n, d):
        out = part[j][n]
        lower, upper = halves(j)
        if d == 2:
            steps[j, n, "turn", 0] = push(out.at[2, lower], turn[j][n].at[0, lower], x_next)
            steps[j, n, "turn", 1] = push(out.at[2, upper], turn[j][n].at[0, upper], x_prev)
        elif d == 1:
            steps[j, n, "got", 0, 1] = push(out.at[1, upper], got[j][n].at[0, upper], x_next)
        elif d == 3:
            steps[j, n, "got", 1, 0] = push(out.at[3, lower], got[j][n].at[1, lower], x_prev)

    def pass_on(j, n):
        if nx == 4:
            lower, upper = halves(j)
            out = part[j][n]
            steps[j, n, "turn", 0].wait_recv()
            out[1, lower] += turn[j][n][0, lower]
            steps[j, n, "turn", 1].wait_recv()
            out[3, upper] += turn[j][n][0, upper]
            steps[j, n, "got", 0, 0] = push(out.at[1, lower], got[j][n].at[0, lower], x_next)
            steps[j, n, "got", 1, 1] = push(out.at[3, upper], got[j][n].at[1, upper], x_prev)

    def finish(j, n):
        value = part[j][n][0]
        if nx == 4:
            for side in (0, 1):
                for half in (0, 1):
                    steps[j, n, "got", side, half].wait_recv()
            value = value + got[j][n][0] + got[j][n][1]
        total[j][n][...] = value
        for p, k in enumerate(row_parts[j]):
            for q in range(nc):
                src = total[j][n].at[p * nc + cmod(q)]
                if k or q:
                    there = plan.device(x, ymod(k), z, cmod(q))
                    steps[n, "back", k, q] = push(src, back[n].at[yc], there)
                else:
                    back[n][yc] = total[j][n][core]

    def hand_over(n):
        for k, q in others:
            steps[n, "back", k, q].wait_recv()
        first = sum(widths[:n])
        for slot in range(nyc):
            h, c = divmod(slot, c_ref.shape[3])
            c_ref[:, :, h, c, first : first + widths[n]] = back[n][slot].reshape(nb, ni, widths[n])

    acts = dict(
        send_b=send_b, b_arrived=b_arrived, ring_arrived=ring_arrived, x_arrived=x_arrived,
        near_arrived=near_arrived, pass_far=pass_far, far_arrived=far_arrived, pair_arrived=pair_arrived,
        product=product, pass_on=pass_on, finish=finish, hand_over=hand_over,
    )
    spread(0)
    cut_a(0, 0, True)
    inner = asrc.shape[2]
    plans = schedule(plan, order, near_first, groups, last_hop, row_parts, chunks, widths, inner)
    for _, act, what in plans[:-1]:
        acts[act](*what)
    for copy in started:
        copy.wait_send()
    acts[plans[-1][1]](*plans[-1][2])


def schedule(plan, order, near_first, groups, last_hop, row_parts, chunks, widths, inner):
    steps, known, free, clock = [], {"go": 0.0}, {}, [0.0]
    rate = 46.0
    piece = 32 * inner * 4 / 1024.0

    def add(act, what, deps, sends=(), cost=0.0, rank=1):
        steps.append((act, what, deps, sends, cost, rank))

    def slot(n):
        return 32 * widths[n] * 4 / 1024.0

    def b_sends(n):
        return [(("b_in", n, k, q), {0: "d", 1: "yu", 2: ("yu", "yd")[q], 3: "yd"}[k], slot(n) * (2 if k == 2 else 1)) for k in [0, *near_first] for q in range(plan.nc) if k or q]

    add("send_b", (0,), ["go"], b_sends(0), 0.0, 0)
    add("x_send", (), [("send_b", 0)], [(("x", k), {1: "xu", 2: "xu", 3: "xd"}[k], piece) for k in order], 0.0, 0)
    for n in chunks[1:]:
        add("send_b", (n,), [("x_send",), ("spread", 0)], b_sends(n), 0.0, 0)

    def spread(k):
        sends = [(("near", k, 3), "yu", piece), (("near", k, 1), "yd", piece)] if near_first else []
        return sends + ([(("pair", k, 0), "d", piece)] if plan.nc > 1 else [])

    add("spread", (0,), [("x_send",)], spread(0), CUT_A, 0)
    for k in order:
        add("x_arrived", (k,), [("x", k)], spread(k), CUT_A, 0)
    all_x = [("x_arrived", k) for k in order]
    cuts = {j: [] for j in range(2)}
    cuts[0] += [("spread", 0), *all_x]
    for k in [0, *order]:
        for ys in [0, *near_first]:
            j = 1 if ys == 2 else 0
            if ys == 2:
                near = ("near_arrived", k, 3 if k in (0, 3) else 1)
                add("pass_far", (k,), [near, *all_x], [(("far", k), "yu" if k in (0, 3) else "yd", piece)], 0.0, 0)
                add("far_arrived", (k,), [("far", k)], [(("pair", k, 2), "d", piece)] if plan.nc > 1 else [], CUT_A, 1)
                cuts[1].append(("far_arrived", k))
            elif ys:
                add("near_arrived", (k, ys), [("near", k, ys)], [(("pair", k, ys), "d", piece)] if plan.nc > 1 else [], CUT_A, 1)
                cuts[0].append(("near_arrived", k, ys))
            if plan.nc > 1:
                add("pair_arrived", (k, ys), [("pair", k, ys)], [], CUT_A, 2)
                cuts[j].append(("pair_arrived", k, ys))
    b_cuts = {n: [] for n in chunks}
    for n in chunks:
        for g, (_, slots, _, pieces) in enumerate(groups[n]):
            keys = [("send_b", n), *(("b_in", n, *piece) for piece in pieces)]
            if n and plan.nz == 8 and plan.ny == 4:
                keys.append(("ring_arrived", *HOLD[n]))
            if g:
                keys.append(("b_arrived", n, g - 1))
            ups = [up for up in (True, False) if last_hop(n, g, up)]
            last = g == len(groups[n]) - 1
            sends = [(("ring", n, g, up, 1), "zu" if up else "zd", slot(n) * slots) for up in ups]
            add("b_arrived", (n, g), keys, sends, CUT_B * last, 0)
            if last:
                b_cuts[n].append(("b_arrived", n, g))
            for hop in range(1, max(last_hop(n, g, True), last_hop(n, g, False)) + 1):
                keys = [("ring", n, g, up, hop) for up in ups if hop <= last_hop(n, g, up)]
                if g:
                    keys.append(("ring_arrived", n, g - 1, hop))
                sends = [(("ring", n, g, up, hop + 1), "zu" if up else "zd", slot(n) * slots) for up in ups if hop < last_hop(n, g, up)]
                add("ring_arrived", (n, g, hop), keys, sends, CUT_B * last * (1 if 2 * hop == plan.nz else 2), 0)
                if last:
                    b_cuts[n].append(("ring_arrived", n, g, hop))
    for n in chunks:
        for j in range(2):
            slots = len(row_parts[j]) * plan.nc
            if not slots:
                continue
            half = slot(n) * slots / 2
            before = cuts[j] + b_cuts[n]
            sets = [(0,)]
            if plan.nx == 4:
                sets = GROUPS[j, n]
            for ds in sets:
                columns = 256 * (-(-2 * widths[n] // 256) + -(-widths[n] // 256))
                cost = 0.25 + DOT * len(ds) * slots * 32 * columns * inner / 1e6
                sends = []
                for d in ds:
                    if d == 2:
                        sends += [(("turn", j, n, 0), "xu", half), (("turn", j, n, 1), "xd", half)]
                    elif d:
                        sends += [(("got", j, n, d, 0), "xu" if d == 1 else "xd", half)]
                add("product", (j, n, ds), before, ["late", *sends], cost, 6 + n - 0.5 * j)
                before = [*before, ("product", j, n, ds)]
            done = before[-1]
            keys = []
            if plan.nx == 4:
                add("pass_on", (j, n), [("turn", j, n, 0), ("turn", j, n, 1), ("product", j, n, next(ds for ds in sets if 3 in ds))], ["late", (("got", j, n, 1, 1), "xu", half), (("got", j, n, 3, 1), "xd", half)], 0.2, 3)
                keys = [("got", j, n, d, i) for d in (1, 3) for i in (0, 1)] + [("pass_on", j, n)]
            sends = ["late"] + [(("back", n, k, q), {0: "d", 1: "yu", 2: ("yu", "yd")[q], 3: "yd"}[k], slot(n) * (2 if k == 2 else 1)) for k in row_parts[j] for q in range(plan.nc) if k or q]
            add("finish", (j, n), [*keys, done], sends, 0.3, 3)
        ends = [("finish", j, n) for j in range(2) if row_parts[j]]
        pieces = [(k, q) for k in [0, *near_first] for q in range(plan.nc) if k or q]
        add("hand_over", (n,), [*ends, *(("back", n, *piece) for piece in pieces)], [], 0.3, 4 + n)

    out = []
    while steps:
        able = [(max(known[d] for d in s[2]), i) for i, s in enumerate(steps) if all(d in known for d in s[2])]
        now = [(steps[i][5], when, i) for when, i in able if when <= clock[0]]
        i = min(now)[2] if now else min(able)[1]
        act, what, deps, sends, cost, _ = steps.pop(i)
        clock[0] = max(clock[0], max(known[d] for d in deps)) + 0.05
        late = bool(sends) and sends[0] == "late"
        if late:
            clock[0] += cost
        for key, link, size in sends[1:] if late else sends:
            speed = 300.0 if link == "d" else rate * 1024 / 1000 * 0.98
            begun = max(clock[0], free.get(link, 0.0))
            free[link] = begun + size / speed
            known[key] = free[link] + (0.9 if link == "d" else LAG)
        if not late:
            clock[0] += cost
        known[(act, *what)] = clock[0]
        out.append((clock[0], act, what))
    first = (("send_b", (0,)), ("x_send", ()), ("spread", (0,)))
    return [(when, act, what) for when, act, what in out if (act, what) not in first]


def exchange_product(plan, widths, a_rows, b_rows):
    nx, nz, nc, nyc = plan.nx, plan.nz, plan.nc, plan.nyc
    nb, ni, nh, na, deep = a_rows.shape
    inner = nh * na * deep // nx
    f32, bf16 = jnp.float32, jnp.bfloat16
    slots = [min(3, plan.ny) * nc, nc] if plan.ny == 4 else [nyc, nc]

    def per_part(of):
        return [[pltpu.VMEM(of(s, w), f32) for w in widths] for s in slots]

    return pl.pallas_call(
        functools.partial(kernel, plan),
        out_shape=pltpu.VMEM(b_rows.shape, f32),
        in_specs=[pl.BlockSpec(memory_space=pl.ANY)] * 2,
        out_specs=pl.BlockSpec(memory_space=pltpu.VMEM),
        scratch_shapes=[
            pltpu.VMEM((nx, 32, inner), f32),
            pltpu.VMEM((nx, nyc, 32, inner), f32),
            [pltpu.VMEM((nx, s * 32, inner), bf16) for s in slots],
            [pltpu.VMEM((nx, s * 32, inner), bf16) for s in slots],
            [pltpu.VMEM((nyc, nb, ni, w), f32) for w in widths],
            [pltpu.VMEM((nz, nyc, nb, ni, w), f32) for w in widths],
            [pltpu.VMEM((inner, 2 * w), bf16) for w in widths],
            per_part(lambda s, w: (nx, s, 32, w)),
            per_part(lambda s, w: (1, s, 32, w)),
            per_part(lambda s, w: (2, s, 32, w)),
            per_part(lambda s, w: (s, 32, w)),
            [pltpu.VMEM((nyc, 32, w), f32) for w in widths],
            pltpu.VMEM(a_rows.shape, f32),
            pltpu.VMEM(b_rows.shape, f32),
            pltpu.SemaphoreType.DMA((2,)),
            pltpu.SemaphoreType.DMA((240,)),
            pltpu.SemaphoreType.DMA((240,)),
        ],
        compiler_params=pltpu.CompilerParams(
            collective_id=0, has_side_effects=True, vmem_limit_bytes=60 * 1024 * 1024
        ),
    )(a_rows, b_rows)


def solution(mesh):
    plan = Plan(4, 4, mesh.shape["str"] // 4, 2)
    spec = P(None, ("cls", "str"), None, None, None)
    return jax.shard_map(
        functools.partial(exchange_product, plan, WIDTHS),
        mesh=mesh,
        in_specs=(spec, spec),
        out_specs=spec,
        check_vma=False,
    )
```
